256 devices in a mesh: span: 32 (over z_hi, y, x_hi), cols: 2 (over z_lo), copy: 4 (over x_lo, core).
Axes of the slice: x: 4 (x_hi: 2, x_lo: 2; x = x_hi * 2 + x_lo), y: 4, z: 8 (z_hi: 4, z_lo: 2; z = z_hi * 2 + z_lo), core: 2. Of those that a mesh axis runs over, the one named last changes fastest.
Arguments:
- leak_rate: float32 [8, 4096, 2560], P('copy', 'span', 'cols'), parts along dimension 0, may hold values from 0.2 to 2
- signal_in: bfloat16 [8, 4096, 2560], P('copy', 'span', 'cols'), parts along dimension 0, may hold values from -6 to 6
- gate_in: bfloat16 [8, 4096, 2560], P('copy', 'span', 'cols'), parts along dimension 0, may hold values from -6 to 6
Outputs:
- sequence_out: bfloat16 [8, 4096, 2560], P('copy', 'span', 'cols'), parts along dimension 0
The draws below stay inside these ranges and needn't reach their ends.
There are 4 independent parts, one for each index of `copy`. The reference program is written for one: setup_inputs(seed, part) draws one part's arguments, and reference() takes and returns one part's arrays. A program takes and returns all parts, laid end to end along the dimension named above; each array names one. Nothing has to cross between parts.
All inputs are finite; a program needn't handle non-finite values.
Results may differ from the reference program's by a relative error of at most 0.001.
Values sent between devices are 32-bit elements; how exact they have to be, the bound alone decides.
A program may use at most 64 MiB of HBM per device.

```python
import jax
import jax.numpy as jnp
from jax import lax

BATCH = 2
CHANNELS = 2560
LENGTH = 4096


def shard_levels(rng, dims, cuts, least, high):
    level = 1.0
    for axis_at, shards_of in cuts:
        draws = jax.random.uniform(jax.random.fold_in(jax.random.fold_in(rng, 6), axis_at), (shards_of,), jnp.float32, least / len(cuts), high / len(cuts))
        level = level * jnp.repeat(jnp.exp(draws), dims[axis_at] // shards_of).reshape((-1,) + (1,) * (len(dims) - 1 - axis_at))
    return level


def noise(stream_key, shape, spread, reach, cuts=(), kind=jnp.bfloat16):
    factor_of = shard_levels(stream_key, shape, cuts, -0.22, 0.18) if cuts else 1.0
    result = jax.random.normal(stream_key, shape, jnp.float32) * spread * factor_of
    return jnp.minimum(jnp.maximum(result, -reach), reach).astype(kind)


def setup_inputs(seed: int = 0, part: int = 0) -> dict:
    arg_keys = jax.random.split(jax.random.key(seed), 4)
    part_splits = jax.random.split(jax.random.fold_in(arg_keys[3], part), 4)
    leak_rate = jnp.clip(0.2 + 1.8 * jax.random.uniform(part_splits[0], (BATCH, LENGTH, CHANNELS), jnp.float32) ** shard_levels(part_splits[0], (BATCH, LENGTH, CHANNELS), ((1, 32), (2, 2)), -0.2, 0.2), 0.2, 2.0)
    signal_in = noise(part_splits[1], (BATCH, LENGTH, CHANNELS), 1.0, 6.0, ((1, 32), (2, 2)))
    gate_in = noise(part_splits[2], (BATCH, LENGTH, CHANNELS), 1.0, 6.0, ((1, 32), (2, 2)))
    return dict(leak_rate=leak_rate, signal_in=signal_in, gate_in=gate_in)


def join_pair(earlier, later):
    return earlier[0] * later[0], later[0] * earlier[1] + later[1]


def reference(leak_rate, signal_in, gate_in):
    keep = jnp.exp(-leak_rate / LENGTH)
    push = signal_in.astype(jnp.float32) * LENGTH ** -0.5
    forward = lax.associative_scan(join_pair, (keep, push), axis=1)[1]
    backward = lax.associative_scan(join_pair, (keep, push), axis=1, reverse=True)[1]
    states = forward + backward
    gated = states * jax.nn.silu(gate_in.astype(jnp.float32))
    sequence_out = gated.astype(jnp.bfloat16)
    return sequence_out
```

```python
import jax
import jax.numpy as jnp
from jax import lax
from jax.experimental import pallas as pl
from jax.experimental.pallas import tpu as pltpu
from jax.sharding import Mesh
from jax.sharding import PartitionSpec as P

SPAN = ("span_0", "span_1", "span_2")
MESH = pl.DeviceIdType.MESH
TILE = 256
LANES = 128
DECAY, FORE, BACK = 0, 1, 2


def kernel(
    length, leak_hbm, signal_hbm, gate_hbm, out_ref,
    leak, signal, gate, keep_fore, keep_back, local, lower, upper, near, mid, far, enter,
    load_sem, gate_sem, send_x, recv_x, send_y, recv_y, send_z, recv_z,
):
    batch, steps, channels = leak.shape
    tiles, groups = channels // TILE, channels // LANES
    z, y, x = (lax.axis_index(name) for name in SPAN)
    axes = (("span_2", x, 2), ("span_1", y, 4), ("span_0", z, 4))

    def load(b, n, which):
        hbm, vmem = ((leak_hbm, leak), (signal_hbm, signal))[which]
        part = (b, slice(None), pl.ds(n * TILE, TILE))
        return pltpu.make_async_copy(hbm.at[part], vmem.at[part], load_sem.at[which, b, n])

    for b in range(batch):
        for n in range(tiles):
            load(b, n, 0).start()
            load(b, n, 1).start()
    gate_load = pltpu.make_async_copy(gate_hbm, gate, gate_sem)
    gate_load.start()

    barrier = pltpu.get_barrier_semaphore()
    for name, mine, size in axes:
        for d in range(1, size):
            pl.semaphore_signal(
                barrier, inc=1, device_id={name: lax.rem(mine + d, size)}, device_id_type=MESH
            )

    row = lax.broadcasted_iota(jnp.int32, (steps, 2 * steps), 0)
    column = lax.rem(lax.broadcasted_iota(jnp.int32, (steps, 2 * steps), 1), steps)
    lower[...] = jnp.where(column <= row, 1.0, 0.0).astype(jnp.bfloat16)
    upper[...] = jnp.where(column >= row, 1.0, 0.0).astype(jnp.bfloat16)

    scale = length ** (-0.5)
    for b in range(batch):
        for n in range(tiles):
            part = (b, slice(None), slice(n * TILE, (n + 1) * TILE))
            load(b, n, 0).wait()
            load(b, n, 1).wait()
            rate = leak[part]
            high = rate.astype(jnp.bfloat16)
            low = (rate - high.astype(jnp.float32)).astype(jnp.bfloat16)
            total = jnp.dot(
                lower[...], jnp.concatenate([high, low], 0), preferred_element_type=jnp.float32
            )
            upto = total * (1.0 / length)
            before = upto - rate * (1.0 / length)
            push = signal[part]
            push_wide = push.astype(jnp.float32)
            grown = (push_wide * (jnp.exp(upto) - 1.0)).astype(jnp.bfloat16)
            shrunk = (push_wide * (jnp.exp(-before) - 1.0)).astype(jnp.bfloat16)
            fore = jnp.dot(
                lower[...], jnp.concatenate([push, grown], 0), preferred_element_type=jnp.float32
            )
            back = jnp.dot(
                upper[...], jnp.concatenate([push, shrunk], 0), preferred_element_type=jnp.float32
            )
            down, up = jnp.exp(-upto), jnp.exp(before)
            fore, back = down * fore * scale, up * back * scale
            keep_fore[part] = down
            keep_back[part] = up
            local[part] = fore + back
            for h in range(TILE // LANES):
                at = b * groups + n * (TILE // LANES) + h
                lanes = slice(h * LANES, (h + 1) * LANES)
                near[x, DECAY, at : at + 1] = upto[steps - 1 :, lanes]
                near[x, FORE, at : at + 1] = fore[steps - 1 :, lanes]
                near[x, BACK, at : at + 1] = back[:1, lanes]

    pl.semaphore_wait(barrier, sum(size - 1 for _, _, size in axes))

    def pass_on(buffer, axis, d, q, slot, send, recv):
        name, mine, size = axis
        return pltpu.make_async_remote_copy(
            src_ref=buffer.at[mine, q],
            dst_ref=buffer.at[mine, q],
            send_sem=send.at[d - 1, slot],
            recv_sem=recv.at[mine, slot],
            device_id={name: lax.rem(mine + d, size)},
            device_id_type=MESH,
        )

    def arrived(buffer, axis, d, q, slot, send, recv):
        name, mine, size = axis
        source = lax.rem(mine + d, size)
        pltpu.make_async_remote_copy(
            src_ref=buffer.at[source, q],
            dst_ref=buffer.at[source, q],
            send_sem=send.at[d - 1, slot],
            recv_sem=recv.at[source, slot],
            device_id={name: source},
            device_id_type=MESH,
        ).wait_recv()

    order = (DECAY, FORE, BACK)
    sent_x = [pass_on(near, axes[0], 1, q, q, send_x, recv_x) for q in order]
    for copy in sent_x:
        copy.start()

    gate_load.wait()
    for b in range(batch):
        for n in range(tiles):
            part = (b, slice(None), slice(n * TILE, (n + 1) * TILE))
            g = gate[part].astype(jnp.float32)
            g = g / (1.0 + jnp.exp(-g))
            keep_fore[part] = keep_fore[part] * g
            keep_back[part] = keep_back[part] * g
            local[part] = local[part] * g

    sent_y, sent_z = [], []
    arrived(near, axes[0], 1, DECAY, DECAY, send_x, recv_x)
    decay = [near[s, DECAY] for s in range(2)]
    mid[y, DECAY] = decay[0] + decay[1]
    kept = [jnp.exp(-d) for d in decay]
    for q in order:
        if q == FORE:
            arrived(near, axes[0], 1, q, q, send_x, recv_x)
            earlier = near[0, FORE]
            mid[y, FORE] = earlier * kept[1] + near[1, FORE]
            carry_fore = jnp.where(x == 1, earlier, 0.0)
            reach_fore = jnp.where(x == 1, kept[0], 1.0)
        if q == BACK:
            arrived(near, axes[0], 1, q, q, send_x, recv_x)
            later = near[1, BACK]
            mid[y, BACK] = later * kept[0] + near[0, BACK]
            carry_back = jnp.where(x == 0, later, 0.0)
            reach_back = jnp.where(x == 0, kept[1], 1.0)
        for d in range(1, 4):
            copy = pass_on(mid, axes[1], d, q, q, send_y, recv_y)
            copy.start()
            sent_y.append(copy)

    for d in range(1, 4):
        arrived(mid, axes[1], d, DECAY, DECAY, send_y, recv_y)
    decay = [mid[s, DECAY] for s in range(4)]
    far[z, DECAY] = (decay[0] + decay[1]) + (decay[2] + decay[3])

    def onward(q, slot, wanted):
        for d in range(1, 4):
            target = lax.rem(z + d, 4)
            copy = pass_on(far, axes[2], d, q, slot, send_z, recv_z)
            if wanted is None:
                copy.start()
            else:
                pl.when(wanted(target))(copy.start)
            if slot == 0 or q == FORE:
                sent_z.append(copy)

    onward(DECAY, 0, None)
    kept = [jnp.exp(-d) for d in decay]
    for d in range(1, 4):
        arrived(mid, axes[1], d, FORE, FORE, send_y, recv_y)
    state, inside, reach = jnp.zeros_like(kept[0]), None, jnp.ones_like(kept[0])
    inside = state
    for s in range(4):
        inside = jnp.where(y == s, state, inside)
        reach = jnp.where(s < y, reach * kept[s], reach)
        state = state * kept[s] + mid[s, FORE]
    far[z, FORE] = state
    onward(FORE, 1, lambda target: target > z)
    carry_fore = carry_fore + reach_fore * inside
    reach_fore = reach_fore * reach
    for d in range(1, 4):
        arrived(mid, axes[1], d, BACK, BACK, send_y, recv_y)
    state, reach = jnp.zeros_like(kept[0]), jnp.ones_like(kept[0])
    inside = state
    for s in reversed(range(4)):
        inside = jnp.where(y == s, state, inside)
        reach = jnp.where(s > y, reach * kept[s], reach)
        state = state * kept[s] + mid[s, BACK]
    far[z, BACK] = state
    onward(BACK, 1, lambda target: target < z)
    carry_back = carry_back + reach_back * inside
    reach_back = reach_back * reach

    for d in range(1, 4):
        arrived(far, axes[2], d, DECAY, 0, send_z, recv_z)
    kept = [jnp.exp(-far[s, DECAY]) for s in range(4)]
    for d in range(1, 4):
        arrived(far, axes[2], d, FORE, 1, send_z, recv_z)
    state = jnp.zeros_like(kept[0])
    for s in range(4):
        state = jnp.where(s < z, state * kept[s] + far[s, FORE], state)
    enter[0] = carry_fore + reach_fore * state
    state = jnp.zeros_like(kept[0])
    for s in reversed(range(4)):
        state = jnp.where(s > z, state * kept[s] + far[s, BACK], state)
    enter[1] = (carry_back + reach_back * state) * jnp.exp(-near[x, DECAY])

    for b in range(batch):
        for n in range(groups):
            part = (b, slice(None), slice(n * LANES, (n + 1) * LANES))
            at = b * groups + n
            fore, back = enter[0, at : at + 1], enter[1, at : at + 1]
            gated = local[part] + (keep_fore[part] * fore + keep_back[part] * back)
            out_ref[part] = gated.astype(jnp.bfloat16)

    for copy in sent_x + sent_y + sent_z:
        copy.wait_send()


def solution(mesh):
    split = Mesh(
        mesh.devices.reshape(4, 4, 2, mesh.shape["cols"], mesh.shape["copy"]),
        ("span_0", "span_1", "span_2", "cols", "copy"),
    )

    def body(leak_rate, signal_in, gate_in):
        shape = leak_rate.shape
        batch, steps, channels = shape
        rows = batch * channels // LANES
        length = steps * lax.axis_size(SPAN)
        wide, narrow = pltpu.VMEM(shape, jnp.float32), pltpu.VMEM(shape, jnp.bfloat16)
        ends = pltpu.VMEM((4, 3, rows, LANES), jnp.float32)
        triangle = pltpu.VMEM((steps, 2 * steps), jnp.bfloat16)
        dma = pltpu.SemaphoreType.DMA
        return pl.pallas_call(
            lambda *refs: kernel(length, *refs),
            out_shape=jax.ShapeDtypeStruct(shape, jnp.bfloat16),
            in_specs=[pl.BlockSpec(memory_space=pl.ANY)] * 3,
            out_specs=pl.BlockSpec(memory_space=pltpu.VMEM),
            scratch_shapes=[
                wide, narrow, narrow, wide, wide, wide, triangle, triangle,
                pltpu.VMEM((2, 3, rows, LANES), jnp.float32), ends, ends,
                pltpu.VMEM((2, rows, LANES), jnp.float32),
                dma((2, batch, channels // TILE)), dma,
                dma((1, 3)), dma((2, 3)), dma((3, 3)), dma((4, 3)), dma((3, 2)), dma((4, 2)),
            ],
            compiler_params=pltpu.CompilerParams(collective_id=0, has_side_effects=True),
        )(leak_rate, signal_in, gate_in)

    placed = (P("copy", SPAN, "cols"),) * 3
    return jax.shard_map(
        body, mesh=split, in_specs=placed, out_specs=P("copy", SPAN, "cols"), check_vma=False
    )
```

```python
import jax
import jax.numpy as jnp
from jax import lax
from jax.experimental import pallas as pl
from jax.experimental.pallas import tpu as pltpu
from jax.sharding import Mesh
from jax.sharding import PartitionSpec as P

SPAN = ("span_0", "span_1", "span_2")
MESH = pl.DeviceIdType.MESH
TILE = 256
LANES = 128
DECAY, FORE, BACK = 0, 1, 2


def kernel(
    length, leak_hbm, signal_hbm, gate_hbm, out_ref,
    leak, signal, gate, keep_fore, keep_back, local, lower, upper, near, mid, far, enter,
    load_sem, gate_sem, send_x, recv_x, send_y, recv_y, send_z, recv_z,
):
    batch, steps, channels = leak.shape
    tiles, groups = channels // TILE, channels // LANES
    z, y, x = (lax.axis_index(name) for name in SPAN)
    axes = (("span_2", x, 2), ("span_1", y, 4), ("span_0", z, 4))

    def load(b, n, which):
        hbm, vmem = ((leak_hbm, leak), (signal_hbm, signal))[which]
        part = (b, slice(None), pl.ds(n * TILE, TILE))
        return pltpu.make_async_copy(hbm.at[part], vmem.at[part], load_sem.at[which, b, n])

    for b in range(batch):
        for n in range(tiles):
            load(b, n, 0).start()
            load(b, n, 1).start()
    gate_load = pltpu.make_async_copy(gate_hbm, gate, gate_sem)
    gate_load.start()

    barrier = pltpu.get_barrier_semaphore()
    for name, mine, size in axes:
        for d in range(1, size):
            pl.semaphore_signal(
                barrier, inc=1, device_id={name: lax.rem(mine + d, size)}, device_id_type=MESH
            )

    row = lax.broadcasted_iota(jnp.int32, (steps, 2 * steps), 0)
    column = lax.rem(lax.broadcasted_iota(jnp.int32, (steps, 2 * steps), 1), steps)
    lower[...] = jnp.where(column <= row, 1.0, 0.0).astype(jnp.bfloat16)
    upper[...] = jnp.where(column >= row, 1.0, 0.0).astype(jnp.bfloat16)

    scale = length ** (-0.5)
    for b in range(batch):
        for n in range(tiles):
            part = (b, slice(None), slice(n * TILE, (n + 1) * TILE))
            load(b, n, 0).wait()
            load(b, n, 1).wait()
            rate = leak[part]
            high = rate.astype(jnp.bfloat16)
            low = (rate - high.astype(jnp.float32)).astype(jnp.bfloat16)
            total = jnp.dot(
                lower[...], jnp.concatenate([high, low], 0), preferred_element_type=jnp.float32
            )
            upto = total * (1.0 / length)
            before = upto - rate * (1.0 / length)
            push = signal[part]
            push_wide = push.astype(jnp.float32)
            grown = (push_wide * (jnp.exp(upto) - 1.0)).astype(jnp.bfloat16)
            shrunk = (push_wide * (jnp.exp(-before) - 1.0)).astype(jnp.bfloat16)
            fore = jnp.dot(
                lower[...], jnp.concatenate([push, grown], 0), preferred_element_type=jnp.float32
            )
            back = jnp.dot(
                upper[...], jnp.concatenate([push, shrunk], 0), preferred_element_type=jnp.float32
            )
            down, up = jnp.exp(-upto), jnp.exp(before)
            fore, back = down * fore * scale, up * back * scale
            keep_fore[part] = down
            keep_back[part] = up
            local[part] = fore + back
            for h in range(TILE // LANES):
                at = b * groups + n * (TILE // LANES) + h
                lanes = slice(h * LANES, (h + 1) * LANES)
                near[x, DECAY, at : at + 1] = upto[steps - 1 :, lanes]
                near[x, FORE, at : at + 1] = fore[steps - 1 :, lanes]
                near[x, BACK, at : at + 1] = back[:1, lanes]

    pl.semaphore_wait(barrier, sum(size - 1 for _, _, size in axes))

    def pass_on(buffer, axis, d, q, slot, send, recv):
        name, mine, size = axis
        return pltpu.make_async_remote_copy(
            src_ref=buffer.at[mine, q],
            dst_ref=buffer.at[mine, q],
            send_sem=send.at[d - 1, slot],
            recv_sem=recv.at[mine, slot],
            device_id={name: lax.rem(mine + d, size)},
            device_id_type=MESH,
        )

    def arrived(buffer, axis, d, q, slot, send, recv):
        name, mine, size = axis
        source = lax.rem(mine + d, size)
        pltpu.make_async_remote_copy(
            src_ref=buffer.at[source, q],
            dst_ref=buffer.at[source, q],
            send_sem=send.at[d - 1, slot],
            recv_sem=recv.at[source, slot],
            device_id={name: source},
            device_id_type=MESH,
        ).wait_recv()

    order = (DECAY, FORE, BACK)
    sent_x = [pass_on(near, axes[0], 1, q, q, send_x, recv_x) for q in order]
    for copy in sent_x:
        copy.start()

    gate_load.wait()
    for b in range(batch):
        for n in range(tiles):
            part = (b, slice(None), slice(n * TILE, (n + 1) * TILE))
            g = gate[part].astype(jnp.float32)
            g = g / (1.0 + jnp.exp(-g))
            keep_fore[part] = keep_fore[part] * g
            keep_back[part] = keep_back[part] * g
            local[part] = local[part] * g

    sent_y, sent_z = [], []
    arrived(near, axes[0], 1, DECAY, DECAY, send_x, recv_x)
    decay = [near[s, DECAY] for s in range(2)]
    mid[y, DECAY] = decay[0] + decay[1]
    kept = [jnp.exp(-d) for d in decay]
    for q in order:
        if q == FORE:
            arrived(near, axes[0], 1, q, q, send_x, recv_x)
            earlier = near[0, FORE]
            mid[y, FORE] = earlier * kept[1] + near[1, FORE]
            carry_fore = jnp.where(x == 1, earlier, 0.0)
            reach_fore = jnp.where(x == 1, kept[0], 1.0)
        if q == BACK:
            arrived(near, axes[0], 1, q, q, send_x, recv_x)
            later = near[1, BACK]
            mid[y, BACK] = later * kept[0] + near[0, BACK]
            carry_back = jnp.where(x == 0, later, 0.0)
            reach_back = jnp.where(x == 0, kept[1], 1.0)
        for d in range(1, 4):
            copy = pass_on(mid, axes[1], d, q, q, send_y, recv_y)
            copy.start()
            sent_y.append(copy)

    for d in range(1, 4):
        arrived(mid, axes[1], d, DECAY, DECAY, send_y, recv_y)
    decay = [mid[s, DECAY] for s in range(4)]
    far[z, DECAY] = (decay[0] + decay[1]) + (decay[2] + decay[3])

    def onward(q, slot, wanted):
        for d in range(1, 4):
            target = lax.rem(z + d, 4)
            copy = pass_on(far, axes[2], d, q, slot, send_z, recv_z)
            if wanted is None:
                copy.start()
            else:
                pl.when(wanted(target))(copy.start)
            if slot == 0 or q == FORE:
                sent_z.append(copy)

    onward(DECAY, 0, None)
    kept = [jnp.exp(-d) for d in decay]
    for d in range(1, 4):
        arrived(mid, axes[1], d, FORE, FORE, send_y, recv_y)
    state, inside, reach = jnp.zeros_like(kept[0]), None, jnp.ones_like(kept[0])
    inside = state
    for s in range(4):
        inside = jnp.where(y == s, state, inside)
        reach = jnp.where(s < y, reach * kept[s], reach)
        state = state * kept[s] + mid[s, FORE]
    far[z, FORE] = state
    onward(FORE, 1, lambda target: target > z)
    carry_fore = carry_fore + reach_fore * inside
    reach_fore = reach_fore * reach
    for d in range(1, 4):
        arrived(mid, axes[1], d, BACK, BACK, send_y, recv_y)
    state, reach = jnp.zeros_like(kept[0]), jnp.ones_like(kept[0])
    inside = state
    for s in reversed(range(4)):
        inside = jnp.where(y == s, state, inside)
        reach = jnp.where(s > y, reach * kept[s], reach)
        state = state * kept[s] + mid[s, BACK]
    far[z, BACK] = state
    onward(BACK, 1, lambda target: target < z)
    carry_back = carry_back + reach_back * inside
    reach_back = reach_back * reach

    for d in range(1, 4):
        arrived(far, axes[2], d, DECAY, 0, send_z, recv_z)
    kept = [jnp.exp(-far[s, DECAY]) for s in range(4)]
    for d in range(1, 4):
        arrived(far, axes[2], d, FORE, 1, send_z, recv_z)
    state = jnp.zeros_like(kept[0])
    for s in range(4):
        state = jnp.where(s < z, state * kept[s] + far[s, FORE], state)
    enter[0] = carry_fore + reach_fore * state
    state = jnp.zeros_like(kept[0])
    for s in reversed(range(4)):
        state = jnp.where(s > z, state * kept[s] + far[s, BACK], state)
    enter[1] = (carry_back + reach_back * state) * jnp.exp(-near[x, DECAY])

    for b in range(batch):
        for n in range(groups):
            part = (b, slice(None), slice(n * LANES, (n + 1) * LANES))
            at = b * groups + n
            fore, back = enter[0, at : at + 1], enter[1, at : at + 1]
            gated = local[part] + (keep_fore[part] * fore + keep_back[part] * back)
            out_ref[part] = gated.astype(jnp.bfloat16)

    for copy in sent_x + sent_y + sent_z:
        copy.wait_send()


def solution(mesh):
    split = Mesh(
        mesh.devices.reshape(4, 4, 2, mesh.shape["cols"], mesh.shape["copy"]),
        ("span_0", "span_1", "span_2", "cols", "copy"),
    )

    def body(leak_rate, signal_in, gate_in):
        shape = leak_rate.shape
        batch, steps, channels = shape
        rows = batch * channels // LANES
        length = steps * lax.axis_size(SPAN)
        wide, narrow = pltpu.VMEM(shape, jnp.float32), pltpu.VMEM(shape, jnp.bfloat16)
        ends = pltpu.VMEM((4, 3, rows, LANES), jnp.float32)
        triangle = pltpu.VMEM((steps, 2 * steps), jnp.bfloat16)
        dma = pltpu.SemaphoreType.DMA
        return pl.pallas_call(
            lambda *refs: kernel(length, *refs),
            out_shape=pltpu.VMEM(shape, jnp.bfloat16),
            in_specs=[pl.BlockSpec(memory_space=pl.ANY)] * 3,
            out_specs=pl.BlockSpec(memory_space=pltpu.VMEM),
            scratch_shapes=[
                wide, narrow, narrow, wide, wide, wide, triangle, triangle,
                pltpu.VMEM((2, 3, rows, LANES), jnp.float32), ends, ends,
                pltpu.VMEM((2, rows, LANES), jnp.float32),
                dma((2, batch, channels // TILE)), dma,
                dma((1, 3)), dma((2, 3)), dma((3, 3)), dma((4, 3)), dma((3, 2)), dma((4, 2)),
            ],
            compiler_params=pltpu.CompilerParams(collective_id=0, has_side_effects=True),
        )(leak_rate, signal_in, gate_in)

    placed = (P("copy", SPAN, "cols"),) * 3
    return jax.shard_map(
        body, mesh=split, in_specs=placed, out_specs=P("copy", SPAN, "cols"), check_vma=False
    )
```

```python
import jax
import jax.numpy as jnp
from jax import lax
from jax.experimental import pallas as pl
from jax.experimental.pallas import tpu as pltpu
from jax.sharding import Mesh
from jax.sharding import PartitionSpec as P

SPAN = ("span_0", "span_1", "span_2")
MESH = pl.DeviceIdType.MESH
TILE, LANES, GROUP = 256, 128, 640
FORE, DECAY, BACK = 0, 1, 2
AROUND = ((2, 1), (1, 1), (3, 1), (2, 0), (0, 1), (1, 0), (3, 0))


def kernel(
    length, leak_hbm, signal_hbm, gate_hbm, out_ref,
    leak, signal, gate, upto_ref, keep_fore, keep_back, local, lower, upper, near, far, enter,
    load_sem, gate_sem, send_near, recv_near, send_far, recv_far,
):
    batch, steps, channels = leak.shape
    groups = channels // LANES
    z, y, x = (lax.axis_index(name) for name in SPAN)
    me = y * 2 + x
    parts = [
        (b, slice(None), slice(c, c + GROUP)) for b in range(batch) for c in range(0, channels, GROUP)
    ]

    def loads(k):
        return [
            pltpu.make_async_copy(hbm.at[parts[k]], vmem.at[parts[k]], load_sem.at[which, k])
            for which, (hbm, vmem) in enumerate(((leak_hbm, leak), (signal_hbm, signal)))
        ]

    for k in range(len(parts)):
        for copy in loads(k):
            copy.start()
    gate_load = pltpu.make_async_copy(gate_hbm, gate, gate_sem)
    gate_load.start()

    def beside(dy, dx):
        return lax.rem(y + dy, 4), lax.rem(x + dx, 2)

    barrier = pltpu.get_barrier_semaphore()
    for dy, dx in AROUND:
        there = beside(dy, dx)
        pl.semaphore_signal(
            barrier, inc=1, device_id={"span_1": there[0], "span_2": there[1]}, device_id_type=MESH
        )
    for d in range(1, 4):
        pl.semaphore_signal(
            barrier, inc=1, device_id={"span_0": lax.rem(z + d, 4)}, device_id_type=MESH
        )

    row = lax.broadcasted_iota(jnp.int32, (steps, 2 * steps), 0)
    column = lax.rem(lax.broadcasted_iota(jnp.int32, (steps, 2 * steps), 1), steps)
    lower[...] = jnp.where(column <= row, 1.0, 0.0).astype(jnp.bfloat16)
    upper[...] = jnp.where(column >= row, 1.0, 0.0).astype(jnp.bfloat16)

    scale = length ** (-0.5)

    def add_up(k):
        rate = leak[parts[k]]
        high = rate.astype(jnp.bfloat16)
        low = (rate - high.astype(jnp.float32)).astype(jnp.bfloat16)
        total = jnp.dot(
            lower[...], jnp.concatenate([high, low], 0), preferred_element_type=jnp.float32
        )
        upto_ref[parts[k]] = total * (1.0 / length)

    def summarize(k):
        upto = upto_ref[parts[k]]
        before = upto - leak[parts[k]] * (1.0 / length)
        push = signal[parts[k]].astype(jnp.float32)
        last = upto[steps - 1 :]
        fore = jnp.sum(jnp.exp(upto) * push, 0, keepdims=True) * (jnp.exp(-last) * scale)
        back = jnp.sum(jnp.exp(-before) * push, 0, keepdims=True) * scale
        for h in range(GROUP // LANES):
            at = k * (GROUP // LANES) + h
            lanes = slice(h * LANES, (h + 1) * LANES)
            near[me, DECAY, at : at + 1] = last[:, lanes]
            near[me, FORE, at : at + 1] = fore[:, lanes]
            near[me, BACK, at : at + 1] = back[:, lanes]

    for k in range(len(parts)):
        for copy in loads(k):
            copy.wait()
        add_up(k)
        if k:
            summarize(k - 1)
    summarize(len(parts) - 1)

    pl.semaphore_wait(barrier, len(AROUND) + 3)

    def to_slab(i, planes, kind):
        there = beside(*AROUND[i])
        return pltpu.make_async_remote_copy(
            src_ref=near.at[me, planes],
            dst_ref=near.at[me, planes],
            send_sem=send_near.at[i, kind],
            recv_sem=recv_near.at[me, kind],
            device_id={"span_1": there[0], "span_2": there[1]},
            device_id_type=MESH,
        )

    def from_slab(i, planes, kind):
        there = beside(*AROUND[i])
        at = there[0] * 2 + there[1]
        pltpu.make_async_remote_copy(
            src_ref=near.at[at, planes],
            dst_ref=near.at[at, planes],
            send_sem=send_near.at[i, kind],
            recv_sem=recv_near.at[at, kind],
            device_id={"span_1": there[0], "span_2": there[1]},
            device_id_type=MESH,
        ).wait_recv()

    first, second = pl.ds(DECAY, 2), pl.ds(FORE, 1)
    sent = [to_slab(i, first, 0) for i in range(len(AROUND))]
    sent += [to_slab(i, second, 1) for i in range(len(AROUND))]
    for copy in sent:
        copy.start()

    gate_load.wait()
    for b in range(batch):
        for c in range(0, channels, TILE):
            part = (b, slice(None), slice(c, c + TILE))
            upto = upto_ref[part]
            before = upto - leak[part] * (1.0 / length)
            push = signal[part]
            push_wide = push.astype(jnp.float32)
            grown = (push_wide * (jnp.exp(upto) - 1.0)).astype(jnp.bfloat16)
            shrunk = (push_wide * (jnp.exp(-before) - 1.0)).astype(jnp.bfloat16)
            fore = jnp.dot(
                lower[...], jnp.concatenate([push, grown], 0), preferred_element_type=jnp.float32
            )
            back = jnp.dot(
                upper[...], jnp.concatenate([push, shrunk], 0), preferred_element_type=jnp.float32
            )
            g = gate[part].astype(jnp.float32)
            g = g / (1.0 + jnp.exp(-g))
            down, up = jnp.exp(-upto) * g, jnp.exp(before) * g
            keep_fore[part] = down
            keep_back[part] = up
            local[part] = (down * fore + up * back) * scale

    def to_slabs(d, planes):
        return pltpu.make_async_remote_copy(
            src_ref=far.at[z, planes],
            dst_ref=far.at[z, planes],
            send_sem=send_far.at[d - 1],
            recv_sem=recv_far.at[z],
            device_id={"span_0": lax.rem(z + d, 4)},
            device_id_type=MESH,
        )

    for i in range(len(AROUND)):
        from_slab(i, first, 0)
    decay = [near[s, DECAY] for s in range(8)]
    kept = [jnp.exp(-d) for d in decay]
    zero = jnp.zeros_like(kept[0])
    state = inside_back = zero
    for s in reversed(range(8)):
        inside_back = jnp.where(me == s, state, inside_back)
        state = state * kept[s] + near[s, BACK]
    far[z, BACK] = state
    far[z, DECAY] = sum(decay[1:], decay[0])
    for d in range(1, 4):
        pl.when(lax.rem(z + d, 4) < z)(to_slabs(d, pl.ds(DECAY, 2)).start)

    for i in range(len(AROUND)):
        from_slab(i, second, 1)
    state = inside_fore = zero
    for s in range(8):
        inside_fore = jnp.where(me == s, state, inside_fore)
        state = state * kept[s] + near[s, FORE]
    far[z, FORE] = state
    for d in range(1, 4):
        pl.when(lax.rem(z + d, 4) > z)(to_slabs(d, pl.ds(FORE, 2)).start)

    ahead = behind = zero
    for s in range(8):
        ahead = jnp.where(me > s, ahead + decay[s], ahead)
        behind = jnp.where(me < s, behind + decay[s], behind)
    own = jnp.exp(-near[me, DECAY])
    reach_fore, reach_back = jnp.exp(-ahead), jnp.exp(-behind) * own
    inside_back = inside_back * own

    for d in range(1, 4):
        source = lax.rem(z + d, 4)
        pltpu.make_async_remote_copy(
            src_ref=far.at[source, pl.ds(DECAY, 2)],
            dst_ref=far.at[source, pl.ds(DECAY, 2)],
            send_sem=send_far.at[d - 1],
            recv_sem=recv_far.at[source],
            device_id={"span_0": source},
            device_id_type=MESH,
        ).wait_recv()
    kept = [jnp.exp(-far[s, DECAY]) for s in range(4)]
    state = zero
    for s in range(4):
        state = jnp.where(s < z, state * kept[s] + far[s, FORE], state)
    enter[0] = inside_fore + reach_fore * state
    state = zero
    for s in reversed(range(4)):
        state = jnp.where(s > z, state * kept[s] + far[s, BACK], state)
    enter[1] = inside_back + reach_back * state

    for b in range(batch):
        for n in range(groups):
            part = (b, slice(None), slice(n * LANES, (n + 1) * LANES))
            at = b * groups + n
            fore, back = enter[0, at : at + 1], enter[1, at : at + 1]
            gated = local[part] + (keep_fore[part] * fore + keep_back[part] * back)
            out_ref[part] = gated.astype(jnp.bfloat16)

    for copy in sent:
        copy.wait_send()
    for d in range(1, 4):
        to_slabs(d, pl.ds(DECAY, 2)).wait_send()


def solution(mesh):
    split = Mesh(
        mesh.devices.reshape(4, 4, 2, mesh.shape["cols"], mesh.shape["copy"]),
        ("span_0", "span_1", "span_2", "cols", "copy"),
    )

    def body(leak_rate, signal_in, gate_in):
        shape = leak_rate.shape
        batch, steps, channels = shape
        rows = batch * channels // LANES
        length = steps * lax.axis_size(SPAN)
        wide, narrow = pltpu.VMEM(shape, jnp.float32), pltpu.VMEM(shape, jnp.bfloat16)
        triangle = pltpu.VMEM((steps, 2 * steps), jnp.bfloat16)
        dma = pltpu.SemaphoreType.DMA
        return pl.pallas_call(
            lambda *refs: kernel(length, *refs),
            out_shape=pltpu.VMEM(shape, jnp.bfloat16),
            in_specs=[pl.BlockSpec(memory_space=pl.ANY)] * 3,
            out_specs=pl.BlockSpec(memory_space=pltpu.VMEM),
            scratch_shapes=[
                wide, narrow, narrow, wide, wide, wide, wide, triangle, triangle,
                pltpu.VMEM((8, 3, rows, LANES), jnp.float32),
                pltpu.VMEM((4, 3, rows, LANES), jnp.float32),
                pltpu.VMEM((2, rows, LANES), jnp.float32),
                dma((2, batch * channels // GROUP)), dma,
                dma((len(AROUND), 2)), dma((8, 2)), dma((3,)), dma((4,)),
            ],
            compiler_params=pltpu.CompilerParams(collective_id=0, has_side_effects=True),
        )(leak_rate, signal_in, gate_in)

    placed = (P("copy", SPAN, "cols"),) * 3
    return jax.shard_map(
        body, mesh=split, in_specs=placed, out_specs=P("copy", SPAN, "cols"), check_vma=False
    )
```

```python
import math

import jax
import jax.numpy as jnp
from jax import lax
from jax.experimental import pallas as pl
from jax.experimental.pallas import tpu as pltpu
from jax.sharding import Mesh
from jax.sharding import PartitionSpec as P

SPAN = ("slab", "place")
MESH = pl.DeviceIdType.MESH
TILE, LANES, GROUP = 256, 128, 640
FORE, DECAY, BACK = 0, 1, 2


def kernel(
    length, leak_hbm, signal_hbm, gate_hbm, out_ref,
    leak, signal, gate, since_ref, keep_fore, keep_back, local, ahead_of, lower, upper, near, far, enter,
    load_sem, near_sem, far_sem,
):
    batch, steps, channels = leak.shape
    groups = channels // LANES
    z, me = lax.axis_index("slab"), lax.axis_index("place")
    parts = [
        (b, slice(None), slice(c, c + GROUP)) for b in range(batch) for c in range(0, channels, GROUP)
    ]

    def load(which, k):
        hbm, vmem = ((leak_hbm, leak), (signal_hbm, signal))[which]
        return pltpu.make_async_copy(hbm.at[parts[k]], vmem.at[parts[k]], load_sem.at[which, k])

    for k in range(len(parts)):
        for which in range(2):
            load(which, k).start()
    gate_load = pltpu.make_async_copy(gate_hbm, gate, load_sem.at[0, 0])
    barrier = pltpu.get_barrier_semaphore()
    for d in range(1, 8):
        pl.semaphore_signal(
            barrier, inc=1, device_id={"place": lax.rem(me + d, 8)}, device_id_type=MESH
        )
    for d in range(1, 4):
        pl.semaphore_signal(
            barrier, inc=1, device_id={"slab": lax.rem(z + d, 4)}, device_id_type=MESH
        )

    row = lax.broadcasted_iota(jnp.int32, (steps, 2 * steps), 0)
    column = lax.rem(lax.broadcasted_iota(jnp.int32, (steps, 2 * steps), 1), steps)
    ahead_of[...] = jnp.where(column < row, -1.0, 0.0).astype(jnp.bfloat16)
    lower[...] = jnp.where(column <= row, 1.0, 0.0).astype(jnp.bfloat16)
    upper[...] = jnp.where(column >= row, 1.0, 0.0).astype(jnp.bfloat16)

    scale = length ** (-0.5)
    rate_scale = math.log2(math.e) / length

    def add_up(k):
        rate = leak[parts[k]]
        high = rate.astype(jnp.bfloat16)
        low = (rate - high.astype(jnp.float32)).astype(jnp.bfloat16)
        total = jnp.dot(
            ahead_of[...], jnp.concatenate([high, low], 0), preferred_element_type=jnp.float32
        )
        since_ref[parts[k]] = total * rate_scale

    def summarize(k):
        b, _, columns = parts[k]
        for h in range(GROUP // LANES):
            at = k * (GROUP // LANES) + h
            start = columns.start + h * LANES
            lanes = slice(start, start + LANES)
            back = jnp.zeros((8, LANES), jnp.float32)
            for r in range(0, steps, 16):
                piece = (b, slice(r, r + 16), lanes)
                reached = jnp.exp2(since_ref[piece]) * signal[piece].astype(jnp.float32)
                back = back + (reached[:8] + reached[8:])
            end = (b, slice(steps - 1, steps), lanes)
            near[me, DECAY, at : at + 1] = leak[end] * rate_scale - since_ref[end]
            near[me, BACK, at : at + 1] = jnp.sum(back, 0, keepdims=True) * scale

    for k in range(len(parts)):
        load(0, k).wait()
        load(1, k).wait()
        add_up(k)
        if k:
            summarize(k - 1)
    summarize(len(parts) - 1)
    gate_load.start()

    pl.semaphore_wait(barrier, 10)

    def within(i, planes, kind):
        return pltpu.make_async_remote_copy(
            src_ref=near.at[me, planes],
            dst_ref=near.at[me, planes],
            send_sem=near_sem.at[2],
            recv_sem=near_sem.at[kind],
            device_id={"place": i},
            device_id_type=MESH,
        )

    def all_within(planes, kind):
        part = near.at[pl.ds(0, 7), planes]
        return pltpu.make_async_remote_copy(
            src_ref=part,
            dst_ref=part,
            send_sem=near_sem.at[2],
            recv_sem=near_sem.at[kind],
            device_id={"place": me},
            device_id_type=MESH,
        )

    first, second = pl.ds(DECAY, 2), pl.ds(FORE, 1)
    for k in range(7):
        within(k + lax.div(k - me + 8, 8), first, 0).start()

    gate_load.wait()
    for b in range(batch):
        for c in range(0, channels, TILE):
            part = (b, slice(None), slice(c, c + TILE))
            since = since_ref[part]
            upto = leak[part] * rate_scale - since
            push = signal[part]
            push_wide = push.astype(jnp.float32)
            growth = jnp.exp2(upto)
            reached = jnp.sum(growth * push_wide, 0, keepdims=True)
            for h in range(TILE // LANES):
                at = b * groups + c // LANES + h
                near[me, FORE, at : at + 1] = reached[:, h * LANES : (h + 1) * LANES]
            grown = (push_wide * (growth - 1.0)).astype(jnp.bfloat16)
            shrunk = (push_wide * (jnp.exp2(since) - 1.0)).astype(jnp.bfloat16)
            fore = jnp.dot(
                lower[...], jnp.concatenate([push, grown], 0), preferred_element_type=jnp.float32
            )
            back = jnp.dot(
                upper[...], jnp.concatenate([push, shrunk], 0), preferred_element_type=jnp.float32
            )
            g = gate[part].astype(jnp.float32)
            g = g / (1.0 + jnp.exp(-g))
            down, up = jnp.exp2(-upto) * g, jnp.exp2(-since) * g
            keep_fore[part] = down
            keep_back[part] = up
            local[part] = (down * fore + up * back) * scale

    own = jnp.exp2(-near[me, DECAY])
    near[me, FORE] = near[me, FORE] * (own * scale)
    for k in range(7):
        within(k + lax.div(k - me + 8, 8), second, 1).start()

    def across(i, planes):
        return pltpu.make_async_remote_copy(
            src_ref=far.at[z, planes],
            dst_ref=far.at[z, planes],
            send_sem=far_sem.at[0],
            recv_sem=far_sem.at[1],
            device_id={"slab": i},
            device_id_type=MESH,
        )

    all_within(first, 0).wait_recv()
    decay = [near[s, DECAY] for s in range(8)]
    kept = [jnp.exp2(-d) for d in decay]
    zero = jnp.zeros_like(kept[0])
    state = inside_back = zero
    for s in reversed(range(8)):
        inside_back = jnp.where(me == s, state, inside_back)
        state = state * kept[s] + near[s, BACK]
    far[z, BACK] = state
    far[z, DECAY] = sum(decay[1:], decay[0])
    for i in range(3):
        pl.when(i < z)(across(i, pl.ds(DECAY, 2)).start)

    all_within(second, 1).wait_recv()
    state = inside_fore = zero
    for s in range(8):
        inside_fore = jnp.where(me == s, state, inside_fore)
        state = state * kept[s] + near[s, FORE]
    far[z, FORE] = state
    for i in range(1, 4):
        pl.when(i > z)(across(i, pl.ds(FORE, 2)).start)

    ahead = behind = zero
    for s in range(8):
        ahead = jnp.where(me > s, ahead + decay[s], ahead)
        behind = jnp.where(me < s, behind + decay[s], behind)
    reach_fore, reach_back = jnp.exp2(-ahead), jnp.exp2(-behind) * own
    inside_back = inside_back * own
    all_within(slice(None), 0).wait_send()

    three = far.at[pl.ds(0, 2)]
    all_across = pltpu.make_async_remote_copy(
        src_ref=three,
        dst_ref=three,
        send_sem=far_sem.at[0],
        recv_sem=far_sem.at[1],
        device_id={"slab": z},
        device_id_type=MESH,
    )
    all_across.wait_recv()
    kept = [jnp.exp2(-far[s, DECAY]) for s in range(4)]
    state = zero
    for s in range(4):
        state = jnp.where(s < z, state * kept[s] + far[s, FORE], state)
    enter[0] = inside_fore + reach_fore * state
    state = zero
    for s in reversed(range(4)):
        state = jnp.where(s > z, state * kept[s] + far[s, BACK], state)
    enter[1] = inside_back + reach_back * state

    for b in range(batch):
        for n in range(groups):
            part = (b, slice(None), slice(n * LANES, (n + 1) * LANES))
            at = b * groups + n
            fore, back = enter[0, at : at + 1], enter[1, at : at + 1]
            gated = local[part] + (keep_fore[part] * fore + keep_back[part] * back)
            out_ref[part] = gated.astype(jnp.bfloat16)

    all_across.wait_send()


def solution(mesh):
    split = Mesh(
        mesh.devices.reshape(4, 8, mesh.shape["cols"], mesh.shape["copy"]),
        ("slab", "place", "cols", "copy"),
    )

    def body(leak_rate, signal_in, gate_in):
        shape = leak_rate.shape
        batch, steps, channels = shape
        rows = batch * channels // LANES
        length = steps * lax.axis_size(SPAN)
        wide, narrow = pltpu.VMEM(shape, jnp.float32), pltpu.VMEM(shape, jnp.bfloat16)
        triangle = pltpu.VMEM((steps, 2 * steps), jnp.bfloat16)
        dma = pltpu.SemaphoreType.DMA
        return pl.pallas_call(
            lambda *refs: kernel(length, *refs),
            out_shape=pltpu.VMEM(shape, jnp.bfloat16),
            in_specs=[pl.BlockSpec(memory_space=pl.ANY)] * 3,
            out_specs=pl.BlockSpec(memory_space=pltpu.VMEM),
            scratch_shapes=[
                wide, narrow, narrow, wide, wide, wide, wide, triangle, triangle, triangle,
                pltpu.VMEM((8, 3, rows, LANES), jnp.float32),
                pltpu.VMEM((4, 3, rows, LANES), jnp.float32),
                pltpu.VMEM((2, rows, LANES), jnp.float32),
                dma((2, batch * channels // GROUP)), dma((3,)), dma((2,)),
            ],
            compiler_params=pltpu.CompilerParams(collective_id=0, has_side_effects=True),
        )(leak_rate, signal_in, gate_in)

    placed = (P("copy", SPAN, "cols"),) * 3
    return jax.shard_map(
        body, mesh=split, in_specs=placed, out_specs=P("copy", SPAN, "cols"), check_vma=False
    )
```

```python
import math

import jax
import jax.numpy as jnp
from jax import lax
from jax.experimental import pallas as pl
from jax.experimental.pallas import tpu as pltpu
from jax.sharding import Mesh
from jax.sharding import PartitionSpec as P

SPAN = ("slab", "place")
MESH = pl.DeviceIdType.MESH
TILE, LANES, GROUP, CHUNK = 256, 128, 640, 2
FORE, DECAY, BACK = 0, 1, 2

AROUND = ((2, 1), (1, 1), (3, 1), (2, 0), (0, 1), (1, 0), (3, 0))


def kernel(
    length, leak_hbm, signal_hbm, gate_hbm, enter, keep_fore, keep_back, local,
    leak, signal, gate, since_ref, ahead_of, lower, upper, near, far,
    load_sem, near_sem, far_sem, later_sem,
):
    batch, steps, channels = leak.shape
    groups = channels // LANES
    z, me = lax.axis_index("slab"), lax.axis_index("place")
    parts = [
        (b, slice(None), slice(c, c + GROUP)) for b in range(batch) for c in range(0, channels, GROUP)
    ]

    def load(which, k):
        hbm, vmem = ((leak_hbm, leak), (signal_hbm, signal))[which]
        return pltpu.make_async_copy(hbm.at[parts[k]], vmem.at[parts[k]], load_sem.at[which, k])

    for k in range(len(parts)):
        for which in range(2):
            load(which, k).start()
    gate_load = pltpu.make_async_copy(gate_hbm, gate, load_sem.at[0, 0])
    barrier = pltpu.get_barrier_semaphore()
    for d in range(1, 8):
        pl.semaphore_signal(
            barrier, inc=1, device_id={"place": lax.rem(me + d, 8)}, device_id_type=MESH
        )
    for i in range(1, 4):

        @pl.when(i > z)
        def _():
            pl.semaphore_signal(barrier, inc=1, device_id={"slab": i}, device_id_type=MESH)


    row = lax.broadcasted_iota(jnp.int32, (steps, 2 * steps), 0)
    column = lax.rem(lax.broadcasted_iota(jnp.int32, (steps, 2 * steps), 1), steps)
    ahead_of[...] = jnp.where(column < row, -1.0, 0.0).astype(jnp.bfloat16)
    lower[...] = jnp.where(column <= row, 1.0, 0.0).astype(jnp.bfloat16)
    upper[...] = jnp.where(column >= row, 1.0, 0.0).astype(jnp.bfloat16)

    scale = length ** (-0.5)
    rate_scale = math.log2(math.e) / length

    def add_up(k):
        rate = leak[parts[k]]
        high = rate.astype(jnp.bfloat16)
        low = (rate - high.astype(jnp.float32)).astype(jnp.bfloat16)
        total = jnp.dot(
            ahead_of[...], jnp.concatenate([high, low], 0), preferred_element_type=jnp.float32
        )
        since_ref[parts[k]] = total * rate_scale

    def summarize(k):
        b, _, columns = parts[k]
        for h in range(GROUP // LANES):
            at = k * (GROUP // LANES) + h
            start = columns.start + h * LANES
            lanes = slice(start, start + LANES)
            back = jnp.zeros((8, LANES), jnp.float32)
            for r in range(0, steps, 16):
                piece = (b, slice(r, r + 16), lanes)
                reached = jnp.exp2(since_ref[piece]) * signal[piece].astype(jnp.float32)
                back = back + (reached[:8] + reached[8:])
            end = (b, slice(steps - 1, steps), lanes)
            near[me, DECAY, at : at + 1] = leak[end] * rate_scale - since_ref[end]
            near[me, BACK, at : at + 1] = jnp.sum(back, 0, keepdims=True) * scale

    for k in range(len(parts)):
        load(0, k).wait()
        load(1, k).wait()
        add_up(k)
        if k:
            summarize(k - 1)
    summarize(len(parts) - 1)
    gate_load.start()

    pl.semaphore_wait(barrier, 7 + z)

    def within(i, planes, kind):
        return pltpu.make_async_remote_copy(
            src_ref=near.at[me, planes],
            dst_ref=near.at[me, planes],
            send_sem=near_sem.at[2],
            recv_sem=near_sem.at[kind],
            device_id={"place": i},
            device_id_type=MESH,
        )

    def all_within(planes, kind):
        part = near.at[pl.ds(0, 7), planes]
        return pltpu.make_async_remote_copy(
            src_ref=part,
            dst_ref=part,
            send_sem=near_sem.at[2],
            recv_sem=near_sem.at[kind],
            device_id={"place": me},
            device_id_type=MESH,
        )

    first, second = pl.ds(DECAY, 2), pl.ds(FORE, 1)
    y, x = lax.div(me, 2), lax.rem(me, 2)
    others = [lax.rem(y + dy, 4) * 2 + lax.rem(x + dx, 2) for dy, dx in AROUND]

    def to_slab(planes, kind):
        for i in range(2):
            pl.when(i != me)(within(i, planes, kind).start)
        for i in others:
            pl.when(i > 1)(within(i, planes, kind).start)

    to_slab(first, 0)

    gate_load.wait()
    for b in range(batch):
        for c in range(0, channels, TILE):
            part = (b, slice(None), slice(c, c + TILE))
            since = since_ref[part]
            upto = leak[part] * rate_scale - since
            push = signal[part]
            push_wide = push.astype(jnp.float32)
            growth = jnp.exp2(upto)
            reached = jnp.sum(growth * push_wide, 0, keepdims=True)
            for h in range(TILE // LANES):
                at = b * groups + c // LANES + h
                near[me, FORE, at : at + 1] = reached[:, h * LANES : (h + 1) * LANES]
            grown = (push_wide * (growth - 1.0)).astype(jnp.bfloat16)
            shrunk = (push_wide * (jnp.exp2(since) - 1.0)).astype(jnp.bfloat16)
            fore = jnp.dot(
                lower[...], jnp.concatenate([push, grown], 0), preferred_element_type=jnp.float32
            )
            back = jnp.dot(
                upper[...], jnp.concatenate([push, shrunk], 0), preferred_element_type=jnp.float32
            )
            g = gate[part].astype(jnp.float32)
            g = g / (1.0 + jnp.exp(-g))
            down, up = jnp.exp2(-upto) * g, jnp.exp2(-since) * g
            keep_fore[part] = down
            keep_back[part] = up
            local[part] = (down * fore + up * back) * scale

    own = jnp.exp2(-near[me, DECAY])
    near[me, FORE] = near[me, FORE] * (own * scale)
    to_slab(second, 1)

    def across(i, planes):
        return pltpu.make_async_remote_copy(
            src_ref=far.at[z, planes],
            dst_ref=far.at[z, planes],
            send_sem=far_sem.at[0],
            recv_sem=far_sem.at[1],
            device_id={"slab": i},
            device_id_type=MESH,
        )

    all_within(first, 0).wait_recv()
    decay = [near[s, DECAY] for s in range(8)]
    kept = [jnp.exp2(-d) for d in decay]
    zero = jnp.zeros_like(kept[0])
    state = inside_back = zero
    for s in reversed(range(8)):
        inside_back = jnp.where(me == s, state, inside_back)
        state = state * kept[s] + near[s, BACK]
    far[z, BACK] = state
    far[z, DECAY] = sum(decay[1:], decay[0])
    for i in range(3):
        pl.when(i < z)(across(i, pl.ds(DECAY, 2)).start)
    for i in range(3):

        @pl.when(i < z)
        def _():
            pl.semaphore_signal(
                later_sem.at[jnp.where(i == z - 1, 0, 1)],
                inc=1, device_id={"slab": i}, device_id_type=MESH,
            )

    all_within(second, 1).wait_recv()
    state = inside_fore = zero
    for s in range(8):
        inside_fore = jnp.where(me == s, state, inside_fore)
        state = state * kept[s] + near[s, FORE]
    far[z, FORE] = state

    @pl.when(z < 3)
    def _():
        pl.semaphore_wait(later_sem.at[0], 1)
        across(lax.rem(z + 1, 4), pl.ds(FORE, 2)).start()

    @pl.when(z < 2)
    def _():
        pl.semaphore_wait(later_sem.at[1], 2 - z)

    for i in range(2, 4):
        pl.when(i > z + 1)(across(i, pl.ds(FORE, 2)).start)

    ahead = behind = zero
    for s in range(8):
        ahead = jnp.where(me > s, ahead + decay[s], ahead)
        behind = jnp.where(me < s, behind + decay[s], behind)
    reach_fore, reach_back = jnp.exp2(-ahead), jnp.exp2(-behind) * own
    inside_back = inside_back * own
    all_within(slice(None), 0).wait_send()

    three = far.at[pl.ds(0, 2)]
    all_across = pltpu.make_async_remote_copy(
        src_ref=three,
        dst_ref=three,
        send_sem=far_sem.at[0],
        recv_sem=far_sem.at[1],
        device_id={"slab": z},
        device_id_type=MESH,
    )
    all_across.wait_recv()
    kept = [jnp.exp2(-far[s, DECAY]) for s in range(4)]
    state = zero
    for s in range(4):
        state = jnp.where(s < z, state * kept[s] + far[s, FORE], state)
    enter[0] = inside_fore + reach_fore * state
    state = zero
    for s in reversed(range(4)):
        state = jnp.where(s > z, state * kept[s] + far[s, BACK], state)
    enter[1] = inside_back + reach_back * state

    all_across.wait_send()


def finish(enter, keep_fore, keep_back, local, out_hbm, out, sem):
    batch, _, channels = out.shape
    groups = channels // LANES

    def store(b, first, last):
        part = (b, slice(None), slice(first * LANES, last * LANES))
        return pltpu.make_async_copy(out.at[part], out_hbm.at[part], sem)

    for at in range(batch * groups):
        b, n = divmod(at, groups)
        part = (b, slice(None), slice(n * LANES, (n + 1) * LANES))
        fore, back = enter[0, at : at + 1], enter[1, at : at + 1]
        gated = local[part] + (keep_fore[part] * fore + keep_back[part] * back)
        out[part] = gated.astype(jnp.bfloat16)
        if n % CHUNK == CHUNK - 1:
            store(b, n + 1 - CHUNK, n + 1).start()
    pltpu.make_async_copy(out, out_hbm, sem).wait()


def solution(mesh):
    split = Mesh(
        mesh.devices.reshape(4, 8, mesh.shape["cols"], mesh.shape["copy"]),
        ("slab", "place", "cols", "copy"),
    )

    def body(leak_rate, signal_in, gate_in):
        shape = leak_rate.shape
        batch, steps, channels = shape
        rows = batch * channels // LANES
        length = steps * lax.axis_size(SPAN)
        wide, narrow = pltpu.VMEM(shape, jnp.float32), pltpu.VMEM(shape, jnp.bfloat16)
        triangle = pltpu.VMEM((steps, 2 * steps), jnp.bfloat16)
        dma = pltpu.SemaphoreType.DMA
        wide_out = pltpu.VMEM(shape, jnp.float32)
        entering = pltpu.VMEM((2, rows, LANES), jnp.float32)
        vmem = pl.BlockSpec(memory_space=pltpu.VMEM)
        states = pl.pallas_call(
            lambda *refs: kernel(length, *refs),
            out_shape=[entering, wide_out, wide_out, wide_out],
            in_specs=[pl.BlockSpec(memory_space=pl.ANY)] * 3,
            out_specs=[vmem] * 4,
            scratch_shapes=[
                wide, narrow, narrow, wide, triangle, triangle, triangle,
                pltpu.VMEM((8, 3, rows, LANES), jnp.float32),
                pltpu.VMEM((4, 3, rows, LANES), jnp.float32),
                dma((2, batch * channels // GROUP)), dma((3,)), dma((2,)),
                pltpu.SemaphoreType.REGULAR((2,)),
            ],
            compiler_params=pltpu.CompilerParams(
                collective_id=0, has_side_effects=True, vmem_limit_bytes=62_600_000
            ),
        )(leak_rate, signal_in, gate_in)
        return pl.pallas_call(
            finish,
            out_shape=jax.ShapeDtypeStruct(shape, jnp.bfloat16),
            in_specs=[vmem] * 4,
            out_specs=pl.BlockSpec(memory_space=pl.ANY),
            scratch_shapes=[narrow, dma],
            compiler_params=pltpu.CompilerParams(vmem_limit_bytes=32 << 20),
        )(*states)

    placed = (P("copy", SPAN, "cols"),) * 3
    return jax.shard_map(
        body, mesh=split, in_specs=placed, out_specs=P("copy", SPAN, "cols"), check_vma=False
    )
```

```python
import math

import jax
import jax.numpy as jnp
from jax import lax
from jax.experimental import pallas as pl
from jax.experimental.pallas import tpu as pltpu
from jax.sharding import Mesh
from jax.sharding import PartitionSpec as P

SPAN = ("slab", "place")
MESH = pl.DeviceIdType.MESH
TILE, LANES, CHUNK = 256, 128, 2
FORE, DECAY, BACK = 0, 1, 2

AROUND = ((2, 1), (1, 1), (3, 1), (2, 0), (0, 1), (1, 0), (3, 0))


def kernel(
    length, leak_hbm, signal_hbm, gate_hbm, enter, keep_back, local,
    leak, signal, gate, since_ref, keep_fore, ahead_of, lower, upper, near, far,
    load_sem, near_sem, far_sem, later_sem,
):
    batch, steps, channels = leak.shape
    groups = channels // LANES
    z, me = lax.axis_index("slab"), lax.axis_index("place")
    parts = [(0, slice(None), slice(0, channels // 2)), (0, slice(None), slice(channels // 2, channels))]
    parts += [(b, slice(None), slice(0, channels)) for b in range(1, batch)]

    for k, part in enumerate(parts):
        pltpu.make_async_copy(leak_hbm.at[part], leak.at[part], load_sem.at[k]).start()
        pltpu.make_async_copy(signal_hbm.at[part], signal.at[part], load_sem.at[k]).start()

    def wait_load(k):
        halves = (parts[k][2].stop - parts[k][2].start) * 2 // channels
        both = leak.at[pl.ds(0, halves), pl.ds(0, steps * 3 // 4)]
        pltpu.make_async_copy(both, both, load_sem.at[k]).wait()

    gate_load = pltpu.make_async_copy(gate_hbm, gate, load_sem.at[0])
    barrier = pltpu.get_barrier_semaphore()
    y, x = lax.div(me, 2), lax.rem(me, 2)
    others = [lax.rem(y + dy, 4) * 2 + lax.rem(x + dx, 2) for dy, dx in AROUND]
    for i in others:
        pl.semaphore_signal(barrier, inc=1, device_id={"place": i}, device_id_type=MESH)
    for i in range(1, 4):

        @pl.when(i > z)
        def _():
            pl.semaphore_signal(barrier, inc=1, device_id={"slab": i}, device_id_type=MESH)


    row = lax.broadcasted_iota(jnp.int32, (steps, 2 * steps), 0)
    column = lax.rem(lax.broadcasted_iota(jnp.int32, (steps, 2 * steps), 1), steps)
    ahead_of[...] = jnp.where(column < row, -1.0, 0.0).astype(jnp.bfloat16)
    lower[...] = jnp.where(column <= row, 1.0, 0.0).astype(jnp.bfloat16)
    upper[...] = jnp.where(column >= row, 1.0, 0.0).astype(jnp.bfloat16)

    scale = length ** (-0.5)
    rate_scale = math.log2(math.e) / length

    def add_up(k):
        rate = leak[parts[k]]
        high = rate.astype(jnp.bfloat16)
        low = (rate - high.astype(jnp.float32)).astype(jnp.bfloat16)
        total = jnp.dot(
            ahead_of[...], jnp.concatenate([high, low], 0), preferred_element_type=jnp.float32
        )
        since_ref[parts[k]] = total * rate_scale

    def summarize(k):
        b, _, columns = parts[k]
        for start in range(columns.start, columns.stop, LANES):
            at = b * groups + start // LANES
            lanes = slice(start, start + LANES)
            back = jnp.zeros((8, LANES), jnp.float32)
            for r in range(0, steps, 16):
                piece = (b, slice(r, r + 16), lanes)
                reached = jnp.exp2(since_ref[piece]) * signal[piece].astype(jnp.float32)
                back = back + (reached[:8] + reached[8:])
            end = (b, slice(steps - 1, steps), lanes)
            near[me, DECAY, at : at + 1] = leak[end] * rate_scale - since_ref[end]
            near[me, BACK, at : at + 1] = jnp.sum(back, 0, keepdims=True) * scale

    for k in range(len(parts)):
        wait_load(k)
        add_up(k)
        if k:
            summarize(k - 1)
    summarize(len(parts) - 1)
    gate_load.start()

    pl.semaphore_wait(barrier, 7 + z)

    def within(i, planes, kind):
        return pltpu.make_async_remote_copy(
            src_ref=near.at[me, planes],
            dst_ref=near.at[me, planes],
            send_sem=near_sem.at[2],
            recv_sem=near_sem.at[kind],
            device_id={"place": i},
            device_id_type=MESH,
        )

    def all_within(planes, kind):
        part = near.at[pl.ds(0, 7), planes]
        return pltpu.make_async_remote_copy(
            src_ref=part,
            dst_ref=part,
            send_sem=near_sem.at[2],
            recv_sem=near_sem.at[kind],
            device_id={"place": me},
            device_id_type=MESH,
        )

    first, second = pl.ds(DECAY, 2), pl.ds(FORE, 1)
    def to_slab(planes, kind):
        for i in range(2):
            pl.when(i != me)(within(i, planes, kind).start)
        for i in others:
            pl.when(i > 1)(within(i, planes, kind).start)

    to_slab(first, 0)

    gate_load.wait()
    for b in range(batch):
        for c in range(0, channels, TILE):
            part = (b, slice(None), slice(c, c + TILE))
            since = since_ref[part]
            upto = leak[part] * rate_scale - since
            push = signal[part]
            push_wide = push.astype(jnp.float32)
            growth = jnp.exp2(upto)
            reached = jnp.sum(growth * push_wide, 0, keepdims=True)
            for h in range(TILE // LANES):
                at = b * groups + c // LANES + h
                near[me, FORE, at : at + 1] = reached[:, h * LANES : (h + 1) * LANES]
            grown = (push_wide * (growth - 1.0)).astype(jnp.bfloat16)
            shrunk = (push_wide * (jnp.exp2(since) - 1.0)).astype(jnp.bfloat16)
            fore = jnp.dot(
                lower[...], jnp.concatenate([push, grown], 0), preferred_element_type=jnp.float32
            )
            back = jnp.dot(
                upper[...], jnp.concatenate([push, shrunk], 0), preferred_element_type=jnp.float32
            )
            g = gate[part].astype(jnp.float32)
            g = g / (1.0 + jnp.exp(-g))
            down, up = jnp.exp2(-upto) * g, jnp.exp2(-since) * g
            keep_fore[part] = down
            keep_back[part] = up
            local[part] = (down * fore + up * back) * scale

    own = jnp.exp2(-near[me, DECAY])
    near[me, FORE] = near[me, FORE] * (own * scale)
    to_slab(second, 1)

    def across(i, kind):
        return pltpu.make_async_remote_copy(
            src_ref=far.at[kind, z],
            dst_ref=far.at[kind, z],
            send_sem=far_sem.at[2],
            recv_sem=far_sem.at[kind],
            device_id={"slab": i},
            device_id_type=MESH,
        )

    all_within(first, 0).wait_recv()
    decay = [near[s, DECAY] for s in range(8)]
    kept = [jnp.exp2(-d) for d in decay]
    zero = jnp.zeros_like(kept[0])
    state = inside_back = zero
    for s in reversed(range(8)):
        inside_back = jnp.where(me == s, state, inside_back)
        state = state * kept[s] + near[s, BACK]
    far[0, z, 1] = state
    far[0, z, 0] = far[1, z, 0] = sum(decay[1:], decay[0])
    for i in range(3):
        pl.when(i < z)(across(i, 0).start)
    for i in range(3):

        @pl.when(i < z)
        def _():
            pl.semaphore_signal(
                later_sem.at[jnp.where(i == z - 1, 0, 1)],
                inc=1, device_id={"slab": i}, device_id_type=MESH,
            )

    all_within(second, 1).wait_recv()
    state = inside_fore = zero
    for s in range(8):
        inside_fore = jnp.where(me == s, state, inside_fore)
        state = state * kept[s] + near[s, FORE]
    far[1, z, 1] = state

    @pl.when(z < 3)
    def _():
        pl.semaphore_wait(later_sem.at[0], 1)
        across(lax.rem(z + 1, 4), 1).start()

    @pl.when(z < 2)
    def _():
        pl.semaphore_wait(later_sem.at[1], 2 - z)

    for i in range(2, 4):
        pl.when(i > z + 1)(across(i, 1).start)

    ahead = behind = zero
    for s in range(8):
        ahead = jnp.where(me > s, ahead + decay[s], ahead)
        behind = jnp.where(me < s, behind + decay[s], behind)
    reach_fore, reach_back = jnp.exp2(-ahead), jnp.exp2(-behind) * own
    inside_back = inside_back * own
    all_within(slice(None), 0).wait_send()

    def all_across(n, kind):
        part = far.at[kind, pl.ds(0, n)]
        return pltpu.make_async_remote_copy(
            src_ref=part,
            dst_ref=part,
            send_sem=far_sem.at[2],
            recv_sem=far_sem.at[kind],
            device_id={"slab": z},
            device_id_type=MESH,
        )

    for n in range(1, 4):
        pl.when(z == n)(all_across(n, 1).wait_recv)
    state = zero
    for s in range(3):
        state = jnp.where(s < z, state * jnp.exp2(-far[1, s, 0]) + far[1, s, 1], state)
    enter[0] = inside_fore + reach_fore * state
    for b in range(batch):
        for n in range(groups):
            part = (b, slice(None), slice(n * LANES, (n + 1) * LANES))
            at = b * groups + n
            local[part] = local[part] + keep_fore[part] * enter[0, at : at + 1]

    for n in range(1, 4):
        pl.when(z == 3 - n)(all_across(n, 0).wait_recv)
    state = zero
    for s in (3, 2, 1):
        state = jnp.where(s > z, state * jnp.exp2(-far[0, s, 0]) + far[0, s, 1], state)
    enter[1] = inside_back + reach_back * state
    all_across(3, 0).wait_send()


def finish(enter, keep_back, local, out_hbm, out, sem):
    batch, _, channels = out.shape
    groups = channels // LANES

    def store(b, first, last):
        part = (b, slice(None), slice(first * LANES, last * LANES))
        return pltpu.make_async_copy(out.at[part], out_hbm.at[part], sem)

    for at in range(batch * groups):
        b, n = divmod(at, groups)
        part = (b, slice(None), slice(n * LANES, (n + 1) * LANES))
        gated = local[part] + keep_back[part] * enter[1, at : at + 1]
        out[part] = gated.astype(jnp.bfloat16)
        if n % CHUNK == CHUNK - 1:
            store(b, n + 1 - CHUNK, n + 1).start()
    pltpu.make_async_copy(out, out_hbm, sem).wait()


def solution(mesh):
    split = Mesh(
        mesh.devices.reshape(4, 8, mesh.shape["cols"], mesh.shape["copy"]),
        ("slab", "place", "cols", "copy"),
    )

    def body(leak_rate, signal_in, gate_in):
        shape = leak_rate.shape
        batch, steps, channels = shape
        rows = batch * channels // LANES
        length = steps * lax.axis_size(SPAN)
        wide, narrow = pltpu.VMEM(shape, jnp.float32), pltpu.VMEM(shape, jnp.bfloat16)
        triangle = pltpu.VMEM((steps, 2 * steps), jnp.bfloat16)
        dma = pltpu.SemaphoreType.DMA
        wide_out = pltpu.VMEM(shape, jnp.float32)
        entering = pltpu.VMEM((2, rows, LANES), jnp.float32)
        vmem = pl.BlockSpec(memory_space=pltpu.VMEM)
        states = pl.pallas_call(
            lambda *refs: kernel(length, *refs),
            out_shape=[entering, wide_out, wide_out],
            in_specs=[pl.BlockSpec(memory_space=pl.ANY)] * 3,
            out_specs=[vmem] * 3,
            scratch_shapes=[
                wide, narrow, narrow, wide, wide, triangle, triangle, triangle,
                pltpu.VMEM((8, 3, rows, LANES), jnp.float32),
                pltpu.VMEM((2, 4, 2, rows, LANES), jnp.float32),
                dma((batch + 1,)), dma((3,)), dma((3,)),
                pltpu.SemaphoreType.REGULAR((2,)),
            ],
            compiler_params=pltpu.CompilerParams(
                collective_id=0, has_side_effects=True, vmem_limit_bytes=63_900_000
            ),
        )(leak_rate, signal_in, gate_in)
        return pl.pallas_call(
            finish,
            out_shape=jax.ShapeDtypeStruct(shape, jnp.bfloat16),
            in_specs=[vmem] * 3,
            out_specs=pl.BlockSpec(memory_space=pl.ANY),
            scratch_shapes=[narrow, dma],
            compiler_params=pltpu.CompilerParams(vmem_limit_bytes=32 << 20),
        )(*states)

    placed = (P("copy", SPAN, "cols"),) * 3
    return jax.shard_map(
        body, mesh=split, in_specs=placed, out_specs=P("copy", SPAN, "cols"), check_vma=False
    )
```
